32 devices in a mesh: row: 4 (over z), col: 8 (over y, x, core).
Axes of the slice: x: 2, y: 2, z: 4, core: 2. Of those that a mesh axis runs over, the one named last changes fastest.
Arguments:
- fock: bfloat16 [18432, 18432], P('row', 'col'), may hold values from -6 to 6
- intersection: bfloat16 [18432, 18432], P('row', 'col'), may hold values from -6 to 6
- tile_mask: int32 [2, 144, 144], P(None, 'row', 'col'), may hold values 0 or 1
- coefficients: bfloat16 [64, 7, 20, 128], P(('row', 'col')), may hold values from -0.5 to 0.5
- domains: int32 [64, 7], P(('row', 'col')), may hold values from 0 to 143, all different within a row; in each aligned block of 16 rows (0 to 15, 16 to 31, ...) at most 2 rows name the same one
- neighbours: int32 [64, 2], P(('row', 'col')), may hold values from 0 to 63, all different within a row
- amplitudes: float32 [64, 20, 20], P(('row', 'col')), may hold values from -0.18 to 0.18
Outputs:
- projected: float32 [64, 20, 20], P(('row', 'col'))
The draws below stay inside these ranges and needn't reach their ends.
Inputs may be any that keep to these rules, and one draw needn't show every extreme that they name: `domains`: each pair names 7 different tiles; among the 16 pairs of one row index (an aligned block of pairs) no tile is named by more than 2 slots. `neighbours`: each pair names 2 different pairs.
All inputs are finite; a program needn't handle non-finite values. No bound on the sum of `tile_mask` on one device may be relied on, other than what follows from the above.
Results may differ from the reference program's by a relative error of at most 0.0041.
Values may be sent and summed in bfloat16 or wider, within the bound.
No kernel may reach another device: no remote copies, remote signals or barrier semaphores. Data moves between devices by JAX's collectives and lax.ppermute only.
A program may use at most 256 MiB of HBM per device.

```python
import math
import jax
import jax.numpy as jnp
import numpy as np
from jax import lax

NT = 144
TILE = 128
NPNO = 20
DT = 7
NB = 2
MOST = 2
GROUP = 16
PAIRS = 64
NPAO = 18432
N_ROW = 4


def set_ends(result, stream_key, smallest, top_value):
    longest = result.shape.index(max(result.shape))
    spots = []
    for shift in (0, 1):
        where = [jax.random.randint(jax.random.fold_in(stream_key, axis), (), 0, length) for axis, length in enumerate(result.shape)]
        where[longest] = (where[longest] + shift) % result.shape[longest]
        spots.append(tuple(where))
    return result.at[spots[0]].set(smallest).at[spots[1]].set(top_value)


def block_levels(stream_key, shape, shards, smallest, largest):
    def one(dim, blocks):
        heights = jax.random.uniform(jax.random.fold_in(jax.random.fold_in(stream_key, 6), dim), (blocks,), jnp.float32, smallest / len(shards), largest / len(shards))
        return jnp.repeat(jnp.exp(heights), shape[dim] // blocks).reshape((-1,) + (1,) * (len(shape) - dim - 1))

    loudness = one(*shards[0])
    for cut in shards[1:]:
        loudness = loudness * one(*cut)
    return loudness


def choose_distinct(key, rows, count, top, lift):
    order = jax.random.permutation(jax.random.fold_in(key, 1), count)
    favour = order
    for power in range(3):
        favour = favour * favour // count
    favour = favour * lift // count
    lots = jax.random.randint(jax.random.fold_in(key, 2), (rows, count), 0, 4096) + favour
    sure = jax.random.permutation(jax.random.fold_in(key, 3), rows)[jnp.arange(count) % rows]
    lots = jnp.where(jnp.arange(rows)[:, None] == sure[None, :], 1 << 14, lots)
    score = lots * count + jnp.arange(count)
    return lax.top_k(score.astype(jnp.int32), top)[1].astype(jnp.int32)


def assign_block(key, own, number, rows, amount, top, most, lean):
    ranking = jax.random.permutation(key, amount)
    packed, usual = load_shares(amount, rows * top, most, lean, True), load_shares(amount, rows * top, most, lean, False)
    places = jnp.arange(amount)

    def named(lengths, offset_by):
        used = int((lengths > 0).sum())
        fixed = max(1, used // 4)
        moved = fixed + (places - fixed + offset_by * (used - fixed)) % max(1, amount - fixed)
        return jnp.zeros((amount,), jnp.int32).at[ranking[jnp.where(places < fixed, places, moved)]].set(jnp.asarray(lengths, jnp.int32))

    lengths = jnp.where(number % 4 == 0, named(packed, number // 4), named(usual, number - number // 4 - 1))
    mixed = jax.random.permutation(jax.random.fold_in(own, 3), amount)
    giver, taker = mixed[0:amount // 2 * 2:2], mixed[1:amount // 2 * 2:2]
    margin = jnp.minimum(lengths[giver] - 1, most - lengths[taker]) // 2
    margin = jnp.where((giver == ranking[0]) | (taker == ranking[0]) | (lengths[taker] == 0), 0, jnp.maximum(margin, 0))
    moved = jax.random.randint(jax.random.fold_in(own, 4), (amount // 2,), 0, 1 << 20) % (margin + 1)
    lengths = lengths.at[giver].add(-moved).at[taker].add(moved)
    labels = jnp.searchsorted(jnp.cumsum(lengths), jnp.arange(rows * top), side="right").astype(jnp.int32)
    table = labels.reshape(top, rows).T
    table = table[jax.random.permutation(jax.random.fold_in(own, 1), rows)]
    offset_by = jax.random.randint(jax.random.fold_in(own, 2), (rows, 1), 0, top)
    return jnp.take_along_axis(table, (jnp.arange(top)[None, :] + offset_by) % top, axis=1)


def load_shares(number_of, total, reach, lean, full):
    weights = [(1 << 20) // math.isqrt(rank ** lean) + 1 for rank in range(1, number_of + 1)]
    largest = reach if full else min(reach, max(-(-total // number_of), total * weights[0] // sum(weights)))
    least = 1 if total - largest >= number_of - 1 else 0
    given, rest = [largest] + [least] * (number_of - 1), total - largest - least * (number_of - 1)
    while rest > 0:
        movable = [i for i in range(1, number_of) if given[i] < largest] or [i for i in range(1, number_of) if given[i] < reach]
        mass, budget = sum([weights[i] for i in movable]), rest
        for i in movable:
            more = min(reach - given[i], max(1, budget * weights[i] // mass), rest)
            given[i] = given[i] + more
            rest = rest - more
    return np.array(given)


def centred(own_key, dims, scale, limit, split=(), kind=jnp.bfloat16):
    entries = jax.random.normal(own_key, dims, jnp.float32) * scale
    if len(split) > 0:
        entries = block_levels(own_key, dims, split, -0.22, 0.18) * entries
    return jnp.clip(entries, min=-limit, max=limit).astype(kind)


def setup_inputs(seed: int = 0) -> dict:
    seeds = jax.random.split(jax.random.key(seed), 8)
    fock = centred(seeds[0], (NPAO, NPAO), 1.0, 6.0, ((0, 4), (1, 8)))
    intersection = centred(seeds[1], (NPAO, NPAO), 1.0, 6.0, ((0, 4), (1, 8)))
    tile_mask = set_ends((jax.random.randint(seeds[2], (2, NT, NT), 0, 2) < 1).astype(jnp.int32), jax.random.fold_in(seeds[2], 1), 0, 1)
    coefficients = centred(seeds[3], (PAIRS, DT, NPNO, TILE), TILE ** -0.5, 0.5, ((0, 32),))
    domains_keys = jax.random.split(jax.random.fold_in(seeds[4], 1), PAIRS // GROUP)
    domains_turns = jax.random.permutation(jax.random.fold_in(seeds[4], 3), PAIRS // GROUP)
    domains = jax.vmap(lambda own, number: assign_block(jax.random.fold_in(seeds[4], 2), own, number, GROUP, NT, DT, MOST, 2))(domains_keys, domains_turns).reshape((PAIRS, DT))
    neighbours = choose_distinct(seeds[5], PAIRS, PAIRS, NB, 256)
    amplitudes = centred(seeds[6], (PAIRS, NPNO, NPNO), 0.03, 0.18, ((0, 32),), jnp.float32)
    return dict(fock=fock, intersection=intersection, tile_mask=tile_mask, coefficients=coefficients, domains=domains, neighbours=neighbours, amplitudes=amplitudes)


HIGH = lax.Precision.HIGHEST


def reference(fock, intersection, tile_mask, coefficients, domains, neighbours, amplitudes):
    tile_rows = NT // N_ROW
    fock_tiles = fock.reshape(NT, TILE, NT, TILE)
    over_tiles = intersection.reshape(NT, TILE, NT, TILE)
    group_ids = jnp.arange(N_ROW).astype(jnp.int32)

    def one_pair(inputs):
        own_coeffs, own_tiles, own_links = inputs
        link_tiles = jnp.take(domains, own_links, axis=0)
        link_coeffs = jnp.take(coefficients, own_links, axis=0)
        rows_index = own_tiles[:, None, None]
        cols_index = link_tiles[None, :, :]
        fock_blocks = fock_tiles[rows_index, :, cols_index, :]
        fock_blocks = fock_blocks * tile_mask[0][rows_index, cols_index].astype(jnp.bfloat16)[..., None, None]
        over_blocks = over_tiles[rows_index, :, cols_index, :]
        over_blocks = over_blocks * tile_mask[1][rows_index, cols_index].astype(jnp.bfloat16)[..., None, None]
        blocks = jnp.stack([fock_blocks, over_blocks], axis=3).astype(jnp.float32)
        parts = jnp.einsum("sak,snumkv->sanumv", own_coeffs.astype(jnp.float32), blocks, precision=HIGH)
        onehot = (group_ids[:, None] == (own_tiles // tile_rows)[None, :]).astype(jnp.float32)
        partial_sum = jnp.einsum("rs,sanumv->ranumv", onehot, parts, precision=HIGH).astype(jnp.bfloat16)
        partial_sum = lax.optimization_barrier(partial_sum).astype(jnp.float32)
        cross = jnp.einsum("ranumv,nubv->nmab", partial_sum, link_coeffs.astype(jnp.float32), precision=HIGH)
        nearby = jnp.take(amplitudes, own_links, axis=0)
        fock_part = cross[:, 0]
        over_part = cross[:, 1]
        first = jnp.einsum("nab,nbc,ndc->ad", over_part, nearby, fock_part, precision=HIGH)
        second = jnp.einsum("nab,nbc,ndc->ad", fock_part, nearby, over_part, precision=HIGH)
        return first + second

    return lax.map(one_pair, (coefficients, domains, neighbours))
```

```python
import functools

import jax
import jax.numpy as jnp
from jax import lax
from jax.experimental import pallas as pl
from jax.experimental.pallas import tpu as pltpu
from jax.sharding import PartitionSpec as P

HIGH = lax.Precision.HIGHEST
UNROLL = 8
RING_BATCHES = 32
ROW_TILE, ROW_SLOT, ROW_COUNT, COL_TILE, COL_SLOT, COL_COUNT, LINK = 0, 8, 16, 24, 32, 40, 48


def cdiv(a, b):
    return -(-a // b)


def pack(coefficients, domains, neighbours, amplitudes):
    pair_dev, per_pair, pno, tile = coefficients.shape
    spread = cdiv(pno, per_pair)
    high = lax.reduce_precision(amplitudes, 8, 7)
    middle = lax.reduce_precision(amplitudes - high, 8, 7)
    low = amplitudes - high - middle
    terms = jnp.concatenate([high, middle, low], axis=2)
    terms = jnp.pad(terms, ((0, 0), (0, per_pair * spread - pno), (0, tile - 3 * pno)))
    terms = terms.reshape(pair_dev, per_pair, spread, tile)
    numbers = jnp.concatenate([domains, neighbours], axis=1)
    numbers = jnp.pad(numbers, ((0, 0), (0, 16 - numbers.shape[1])))
    digits = jnp.concatenate([numbers & 127, numbers >> 7], axis=1)
    digits = jnp.pad(digits, ((0, 0), (0, tile - 32))).astype(jnp.float32)
    digits = jnp.broadcast_to(digits[:, None, None, :], (pair_dev, per_pair, 1, tile))
    rows = pno + spread + 1
    filler = jnp.zeros((pair_dev, per_pair, cdiv(rows, 8) * 8 - rows, tile), jnp.float32)
    extra = jnp.concatenate([terms, filler, digits], axis=2).astype(jnp.bfloat16)
    return jnp.concatenate([coefficients, extra], axis=2).reshape(pair_dev * per_pair, -1, tile)


def xor_send(x, axis, distance):
    size = lax.axis_size(axis)
    return lax.ppermute(x, axis, [(i, i ^ distance) for i in range(size)])


def gather_all(packed, rows, cols):
    mine = jnp.concatenate([packed] + [xor_send(packed, "row", d) for d in range(1, rows)], axis=0)
    unit = mine.shape[0]
    if cols == 8:
        by_x = xor_send(mine, "col", 2)
        by_y = xor_send(mine, "col", 4)
        half = unit // 2
        by_xy_low = xor_send(by_x[:half], "col", 4)
        by_xy_high = xor_send(by_y[half:], "col", 2)
        pieces = [(0, mine), (2 * unit, by_x), (4 * unit, by_y), (6 * unit, by_xy_low), (6 * unit + half, by_xy_high)]
        return pieces + [(first + unit, xor_send(piece, "col", 1)) for first, piece in pieces]
    pieces = [(0, mine)]
    distance = 1
    while distance < cols:
        pieces = pieces + [(first + distance * unit, xor_send(piece, "col", distance)) for first, piece in pieces]
        distance *= 2
    return pieces


def decode_numbers(tile_rows):
    digits = tile_rows.astype(jnp.float32)
    return digits


def project_kernel(cfg, where_ref, mask_ref, fock_ref, over_ref, *refs):
    (firsts, rows, cols, pair_dev, per_pair, links, pno, block_rows, tile, tile_rows, tile_cols) = cfg
    pieces = refs[: len(firsts)]
    out_ref, amp_ref = refs[len(firsts) : len(firsts) + 2]
    (coef, ring, numbers, table_v, table, word_a, word_b, word_c, left, keep_left, keep_out, coef_sem, table_sem, ring_sem) = refs[
        len(firsts) + 2 :
    ]
    devices = rows * cols
    pair_count = devices * pair_dev
    row_index, col_index = where_ref[0], where_ref[1]
    copies = []
    for number, (first, piece) in enumerate(zip(firsts, pieces)):
        copy = pltpu.make_async_copy(piece, coef.at[pl.ds(first, piece.shape[0])], coef_sem.at[number])
        copy.start()
        copies.append(copy)
    out_ref[...] = jnp.zeros_like(out_ref)
    left[...] = jnp.zeros_like(left)
    keep_left[...] = jnp.zeros_like(keep_left)
    keep_out[...] = jnp.zeros_like(keep_out)
    for copy in copies:
        copy.wait()

    for pair in range(pair_count):
        last = coef[pair * per_pair, block_rows - 8 : block_rows, :].astype(jnp.float32)
        numbers[pair : pair + 1, :] = last[7:8, :]

    lane = lax.broadcasted_iota(jnp.int32, (pair_count, tile), 1)
    digits = numbers[...]
    values = digits + 128.0 * pltpu.roll(digits, tile - 16, 1)
    values = jnp.where(lane < 16, values, 0.0)
    is_slot = lane < per_pair
    down = lax.broadcasted_iota(jnp.int32, (tile, tile), 0)
    across = lax.broadcasted_iota(jnp.int32, (tile, tile), 1)
    before = (down < across).astype(jnp.bfloat16)

    def put(values_here, to_lane):
        move = (across == to_lane) & (down < per_pair)
        return jnp.dot(values_here.astype(jnp.bfloat16), move.astype(jnp.bfloat16), preferred_element_type=jnp.float32)

    result = jnp.where((lane >= LINK) & (lane < LINK + links), pltpu.roll(values, LINK - per_pair, 1), 0.0)
    lane_f = lane.astype(jnp.float32)
    for first, extent, at_tile, at_slot, at_count in (
        (row_index * tile_rows, tile_rows, ROW_TILE, ROW_SLOT, ROW_COUNT),
        (col_index * tile_cols, tile_cols, COL_TILE, COL_SLOT, COL_COUNT),
    ):
        local = values - first.astype(jnp.float32)
        valid = is_slot & (local >= 0.0) & (local < float(extent))
        ones = jnp.where(valid, 1.0, 0.0)
        rank = jnp.dot(ones.astype(jnp.bfloat16), before, preferred_element_type=jnp.float32)
        result = result + put(ones, at_count)
        for place in range(per_pair):
            chosen = valid & (rank == float(place))
            result = result + put(jnp.where(chosen, local, 0.0), at_tile + place)
            result = result + put(jnp.where(chosen, lane_f, 0.0), at_slot + place)
    table_v[...] = result.astype(jnp.int32)
    copy = pltpu.make_async_copy(table_v, table, table_sem)
    copy.start()
    copy.wait()

    def fetch(number):
        word = word_a[number]
        upper, lower, column = word & 255, (word >> 8) & 255, (word >> 16) & 255
        slot = lax.rem(number, UNROLL * RING_BATCHES)
        sem = ring_sem.at[slot // UNROLL]
        for half, at in enumerate((upper, lower)):
            for which, matrix in enumerate((fock_ref, over_ref)):
                pltpu.make_async_copy(
                    matrix.at[pl.ds(pl.multiple_of(at * tile, tile), tile), pl.ds(pl.multiple_of(column * tile, tile), tile)],
                    ring.at[slot, half * tile : (half + 1) * tile, which * tile : (which + 1) * tile],
                    sem,
                ).start()

    def add_item(number, a, b, c):
        word_a[number] = a
        word_b[number] = b
        word_c[number] = c

        @pl.when(number < UNROLL * RING_BATCHES)
        def _():
            fetch(number)

    plane = tile_rows * tile_cols

    def one_link(q, carry):
        count, previous = carry
        pair, link = lax.div(q, links), lax.rem(q, links)
        place = lax.div(pair, pair_dev)
        source = (lax.rem(place, rows) ^ row_index) * cols + (lax.div(place, rows) ^ col_index)
        partner = table[pair, LINK + link]
        partner_dev = lax.div(partner, pair_dev)
        partner_place = (lax.rem(partner_dev, cols) ^ col_index) * rows + (lax.div(partner_dev, cols) ^ row_index)
        partner = partner_place * pair_dev + lax.rem(partner, pair_dev)
        row_n = table[pair, ROW_COUNT]
        col_n = table[partner, COL_COUNT]
        chunks = (row_n + 1) >> 1
        lanes = lax.rem(q, pair_dev * links) * pno

        def one_column(u, carry):
            column = table[partner, COL_TILE + u]
            partner_slot = partner * per_pair + table[partner, COL_SLOT + u]
            word_c_here = partner_slot | (lanes << 12) | (source << 20)

            def one_chunk(ch, carry):
                count, previous = carry
                two = jnp.where(2 * ch + 1 < row_n, 1, 0)
                upper = table[pair, ROW_TILE + 2 * ch]
                lower = jnp.where(two == 1, table[pair, ROW_TILE + 2 * ch + 1], upper)
                slot_a = table[pair, ROW_SLOT + 2 * ch]
                slot_b = jnp.where(two == 1, table[pair, ROW_SLOT + 2 * ch + 1], slot_a)
                at_a, at_b = upper * tile_cols + column, lower * tile_cols + column
                flags = (
                    mask_ref[at_a]
                    | (mask_ref[plane + at_a] << 1)
                    | (mask_ref[at_b] << 2)
                    | (mask_ref[plane + at_b] << 3)
                    | (two << 4)
                    | (jnp.where(ch == 0, 1, 0) << 5)
                    | (jnp.where(ch == chunks - 1, 1, 0) << 6)
                )
                fresh = jnp.where(source != previous, 1, 0)
                a = upper | (lower << 8) | (column << 16) | (flags << 24)
                b = (pair * per_pair + slot_a) | ((pair * per_pair + slot_b) << 12) | (fresh << 24)
                add_item(count, a, b, word_c_here)
                return (count + 1, source)

            return lax.fori_loop(0, chunks, one_chunk, carry)

        return lax.fori_loop(0, jnp.where(row_n > 0, col_n, 0), one_column, (count, previous))

    count, last_source = lax.fori_loop(0, pair_count * links, one_link, (jnp.int32(0), jnp.int32(-1)))
    batches = lax.div(count + UNROLL - 1, UNROLL)

    def pad_item(number, carry):
        add_item(number, jnp.int32(1 << 29), jnp.int32(0), jnp.maximum(last_source, 0) << 20)
        return carry

    lax.fori_loop(count, batches * UNROLL, pad_item, 0)

    def first_stage(t):
        base = t * UNROLL
        at = lax.rem(t, RING_BATCHES)
        window = ring.at[pl.ds(at * UNROLL, UNROLL)]
        pltpu.make_async_copy(window, window, ring_sem.at[at]).wait()
        products = []
        for i in range(UNROLL):
            a, b = word_a[base + i], word_b[base + i]
            quads = []
            for half in range(2):
                line = []
                for which in range(2):
                    keep = ((a >> (24 + 2 * half + which)) & 1) == 1
                    block = ring[at * UNROLL + i, half * tile : (half + 1) * tile, which * tile : (which + 1) * tile]
                    line.append(jnp.where(keep, block, jnp.zeros_like(block)))
                quads.append(jnp.concatenate(line, axis=1))
            weights = jnp.concatenate(quads, axis=0)
            upper = coef[b & 4095]
            lower = coef[(b >> 12) & 4095]
            lower = jnp.where(((a >> 28) & 1) == 1, lower, jnp.zeros_like(lower))
            products.append(
                jnp.dot(jnp.concatenate([upper, lower], axis=1), weights, preferred_element_type=jnp.float32)
            )
        running = keep_left[...]
        side = lax.rem(t, 2)
        for i in range(UNROLL):
            a = word_a[base + i]
            running = jnp.where(((a >> 29) & 1) == 1, products[i], running + products[i])
            done = jnp.where(((a >> 30) & 1) == 1, running, jnp.zeros_like(running)).astype(jnp.bfloat16)
            left[side, i, 0:block_rows, :] = done[:, :tile]
            left[side, i, 32 : 32 + block_rows, :] = done[:, tile:]
        keep_left[...] = running

    def second_stage(t):
        base = t * UNROLL
        side = lax.rem(t, 2)
        lanes_here = lax.broadcasted_iota(jnp.int32, (64, tile), 1)
        running = keep_out[...]
        results = []
        for i in range(UNROLL):
            c = word_c[base + i]
            partner = coef[c & 4095]
            result = lax.dot_general(
                left[side, i], partner, (((1,), (1,)), ((), ())), preferred_element_type=jnp.float32
            )
            result = jnp.concatenate([result, jnp.zeros((64, tile - block_rows), jnp.float32)], axis=1)
            result = jnp.where(lanes_here < pno, result, 0.0)
            results.append(pltpu.roll(result, (c >> 12) & 127, 1))
        for i in range(UNROLL):
            b, c = word_b[base + i], word_c[base + i]
            running = jnp.where(((b >> 24) & 1) == 1, results[i], running + results[i])
            both = jnp.concatenate([running[0:block_rows], running[32 : 32 + block_rows]], axis=0)
            out_ref[c >> 20] = both.astype(out_ref.dtype)
        keep_out[...] = running

    def step(t, carry):
        @pl.when(t < batches)
        def _():
            first_stage(t)

            @pl.when(t + RING_BATCHES < batches)
            def _():
                def again(i, carry):
                    fetch((t + RING_BATCHES) * UNROLL + i)
                    return carry

                lax.fori_loop(0, UNROLL, again, 0)

        @pl.when(t > 0)
        def _():
            second_stage(t - 1)

        return carry

    lax.fori_loop(0, jnp.where(batches > 0, batches + 1, 0), step, 0)

    for q in range(pair_dev * links):
        partner = table[q // links, LINK + q % links]
        partner_dev = lax.div(partner, pair_dev)
        partner_place = (lax.rem(partner_dev, cols) ^ col_index) * rows + (lax.div(partner_dev, cols) ^ row_index)
        partner = partner_place * pair_dev + lax.rem(partner, pair_dev)
        for s in range(per_pair):
            amp_ref[q, s] = coef[partner * per_pair + s, 16:block_rows, :].astype(jnp.float32)


def finish_kernel(cfg, got_ref, amp_ref, out_ref):
    (pair_dev, per_pair, links, pno, block_rows, tile) = cfg
    total = jnp.sum(got_ref[...].astype(jnp.float32), axis=0)
    spread = cdiv(pno, per_pair)
    skip = pno - 16
    for pair in range(pair_dev):
        answer = jnp.zeros((pno, pno), jnp.float32)
        for link in range(links):
            q = pair * links + link
            lines = jnp.concatenate([amp_ref[q, s, skip : skip + spread, :] for s in range(per_pair)], axis=0)
            lines = (lines + pltpu.roll(lines, tile - pno, 1)) + pltpu.roll(lines, tile - 2 * pno, 1)
            amps = lines[:pno, :pno]
            moved = total if q == 0 else pltpu.roll(total, tile - q * pno, 1)
            fock_part = moved[0:pno, :pno]
            over_part = moved[block_rows : block_rows + pno, :pno]
            for one, other in ((over_part, fock_part), (fock_part, over_part)):
                inner = jnp.dot(one, amps, precision=HIGH, preferred_element_type=jnp.float32)
                answer = answer + lax.dot_general(
                    inner, other, (((1,), (1,)), ((), ())), precision=HIGH, preferred_element_type=jnp.float32
                )
        out_ref[pair] = answer


def shards(fock, intersection, tile_mask, coefficients, domains, neighbours, amplitudes):
    rows, cols = lax.axis_size("row"), lax.axis_size("col")
    devices = rows * cols
    pair_dev, per_pair, pno, tile = coefficients.shape
    links = neighbours.shape[1]
    tile_rows, tile_cols = fock.shape[0] // tile, fock.shape[1] // tile
    packed = pack(coefficients, domains, neighbours, amplitudes)
    block_rows = packed.shape[1]
    pieces = gather_all(packed, rows, cols)
    firsts = tuple(first for first, _ in pieces)
    place = jnp.stack([lax.axis_index("row"), lax.axis_index("col")]).astype(jnp.int32)
    pair_count = devices * pair_dev
    slots = pair_count * per_pair
    most = pair_count * links * per_pair * cdiv(per_pair, 2) + UNROLL
    cfg = (firsts, rows, cols, pair_dev, per_pair, links, pno, block_rows, tile, tile_rows, tile_cols)
    smem = pl.BlockSpec(memory_space=pltpu.SMEM)
    anywhere = pl.BlockSpec(memory_space=pl.ANY)
    vmem = pl.BlockSpec(memory_space=pltpu.VMEM)
    parts, amp_rows = pl.pallas_call(
        functools.partial(project_kernel, cfg),
        out_shape=(
            jax.ShapeDtypeStruct((devices, 2 * block_rows, tile), jnp.bfloat16),
            jax.ShapeDtypeStruct((pair_dev * links, per_pair, block_rows - 16, tile), jnp.float32),
        ),
        in_specs=[smem, smem, anywhere, anywhere] + [anywhere] * len(pieces),
        out_specs=(vmem, vmem),
        scratch_shapes=[
            pltpu.VMEM((slots, block_rows, tile), jnp.bfloat16),
            pltpu.VMEM((UNROLL * RING_BATCHES, 2 * tile, 2 * tile), jnp.bfloat16),
            pltpu.VMEM((pair_count, tile), jnp.float32),
            pltpu.VMEM((pair_count, tile), jnp.int32),
            pltpu.SMEM((pair_count, tile), jnp.int32),
            pltpu.SMEM((most,), jnp.int32),
            pltpu.SMEM((most,), jnp.int32),
            pltpu.SMEM((most,), jnp.int32),
            pltpu.VMEM((2, UNROLL, 64, tile), jnp.bfloat16),
            pltpu.VMEM((block_rows, 2 * tile), jnp.float32),
            pltpu.VMEM((64, tile), jnp.float32),
            pltpu.SemaphoreType.DMA((len(pieces),)),
            pltpu.SemaphoreType.DMA,
            pltpu.SemaphoreType.DMA((RING_BATCHES,)),
        ],
        compiler_params=pltpu.CompilerParams(vmem_limit_bytes=60 * 1024 * 1024),
    )(place, tile_mask.reshape(-1), fock, intersection, *[piece for _, piece in pieces])
    got = lax.all_to_all(parts, ("row", "col"), 0, 0, tiled=True)
    return pl.pallas_call(
        functools.partial(finish_kernel, (pair_dev, per_pair, links, pno, block_rows, tile)),
        out_shape=jax.ShapeDtypeStruct((pair_dev, pno, pno), jnp.float32),
        in_specs=[vmem, vmem],
        out_specs=vmem,
    )(got, amp_rows)


def solution(mesh):
    placed = (
        P("row", "col"),
        P("row", "col"),
        P(None, "row", "col"),
        P(("row", "col"), None, None, None),
        P(("row", "col"), None),
        P(("row", "col"), None),
        P(("row", "col"), None, None),
    )
    return jax.shard_map(
        shards, mesh=mesh, in_specs=placed, out_specs=P(("row", "col"), None, None), check_vma=False
    )
```
